256 devices in a mesh: lon: 64 (over y_hi, x, z), lat: 4 (over y_lo, core).
Axes of the slice: x: 4, y: 4 (y_hi: 2, y_lo: 2; y = y_hi * 2 + y_lo), z: 8, core: 2. Of those that a mesh axis runs over, the one named last changes fastest.
Arguments:
- increment: bfloat16 [2048, 512, 128], P('lon', 'lat'), may hold values from -6 to 6
- jacobian: bfloat16 [4096, 128, 3072], P(('lon', 'lat')), may hold values from -0.0625 to 0.0625
- lat_weight: float32 [4096, 8], P(('lon', 'lat')), may hold values from 0.2 to 2
- centre: int32 [4096], P(('lon', 'lat')), may hold values from 0 to 31
- west: int32 [4096], P(('lon', 'lat')), may hold values from 0 to 32
- east: int32 [4096], P(('lon', 'lat')), may hold values from 0 to 32
- lat_offset: int32 [4096], P(('lon', 'lat')), may hold values from 0 to 504
- lev_offset: int32 [4096], P(('lon', 'lat')), may hold values from 0 to 96
Outputs:
- departures: float32 [4096, 128], P(('lon', 'lat'))
The draws below stay inside these ranges and needn't reach their ends.
All inputs are finite; a program needn't handle non-finite values.
Results may differ from the reference program's by a relative error of at most 0.0029.
Values may be sent and summed in bfloat16 or wider, within the bound.
No kernel may reach another device: no remote copies, remote signals or barrier semaphores. Data moves between devices by JAX's collectives and lax.ppermute only.
A program may use at most 128 MiB of HBM per device.

```python
import math
import jax
import jax.numpy as jnp
from jax import lax

LON_DEV = 32
SLOTS = 16
LEV = 128
NTAN = 128
BLAT = 8
BLEV = 32
LON = 2048
LAT = 512
SCANS = 4096
N_LON = 64
N_LAT = 4


def place_ends(entries, key, least, largest):
    dims = entries.shape
    spot = [jax.random.randint(jax.random.fold_in(key, axis), (), 0, dims[axis]) for axis in range(len(dims))]
    entries = entries.at[tuple(spot)].set(least)
    longest = dims.index(max(dims))
    spot[longest] = (spot[longest] + 1) % dims[longest]
    return entries.at[tuple(spot)].set(largest)


def level_of(own_key, dims, pieces, low, high):
    factor_of, own = 1.0, jax.random.fold_in(own_key, 6)
    for dim, shards_of in pieces:
        heights = jnp.exp(jax.random.uniform(jax.random.fold_in(own, dim), (shards_of,), jnp.float32, low / len(pieces), high / len(pieces)))
        factor_of = factor_of * jnp.repeat(heights, dims[dim] // shards_of).reshape([-1 if axis == dim else 1 for axis in range(len(dims))])
    return factor_of


def scatter_about(own_key, dims, deviation, bound, pieces=(), held_as=jnp.bfloat16):
    entries = deviation * jax.random.normal(own_key, dims, jnp.float32)
    if pieces:
        entries = entries * level_of(own_key, dims, pieces, -0.22, 0.18)
    return jnp.clip(entries, -bound, bound).astype(held_as)


def setup_inputs(seed: int = 0) -> dict:
    splits = jax.random.split(jax.random.key(seed), 9)
    return {
        "increment": scatter_about(splits[0], (LON, LAT, LEV), 1.0, 6.0, ((0, 64), (1, 4))),
        "jacobian": scatter_about(splits[1], (SCANS, NTAN, 3 * LON_DEV * BLEV), (BLAT * LON_DEV * BLEV) ** -0.5, 0.0625, ((0, 256),)),
        "lat_weight": jnp.clip(jnp.exp(math.log(2.0) - 2.3025851 * jax.random.uniform(splits[2], (SCANS, BLAT), jnp.float32) ** level_of(splits[2], (SCANS, BLAT), ((0, 256),), -0.2, 0.2)), 0.2, 2.0),
        "centre": place_ends(jax.random.randint(splits[3], (SCANS,), 0, LON_DEV), jax.random.fold_in(splits[3], 1), 0, LON_DEV - 1).astype(jnp.int32),
        "west": place_ends(jax.random.randint(splits[4], (SCANS,), 0, LON_DEV + 1), jax.random.fold_in(splits[4], 1), 0, LON_DEV).astype(jnp.int32),
        "east": place_ends(jax.random.randint(splits[5], (SCANS,), 0, LON_DEV + 1), jax.random.fold_in(splits[5], 1), 0, LON_DEV).astype(jnp.int32),
        "lat_offset": place_ends(jax.random.randint(splits[6], (SCANS,), 0, LAT - BLAT + 1), jax.random.fold_in(splits[6], 1), 0, LAT - BLAT).astype(jnp.int32),
        "lev_offset": place_ends(jax.random.randint(splits[7], (SCANS,), 0, LEV - BLEV + 1), jax.random.fold_in(splits[7], 1), 0, LEV - BLEV).astype(jnp.int32),
    }


def reference(increment, jacobian, lat_weight, centre, west, east, lat_offset, lev_offset):
    span = 3 * LON_DEV
    longitude = LON_DEV * N_LON

    def one_scan(item):
        index, kmat, weights, mid, left, right, lat_first, lev_first = item
        sector = index // (SLOTS * N_LAT)
        rows = jnp.arange(span, dtype=jnp.int32)
        columns = ((sector * LON_DEV - LON_DEV + rows) % longitude).astype(jnp.int32)
        window = jnp.take(increment, columns, axis=0)
        zero = jnp.zeros((), jnp.int32)
        box = lax.dynamic_slice(window, (zero, lat_first.astype(jnp.int32), lev_first.astype(jnp.int32)), (span, BLAT, BLEV))
        profile = jnp.einsum("rjk,j->rk", box.astype(jnp.float32), weights.astype(jnp.float32), precision=lax.Precision.HIGHEST)
        keep = (rows >= LON_DEV + mid - left) & (rows <= LON_DEV + mid + right)
        profile = jnp.where(keep[:, None], profile, jnp.zeros_like(profile)).astype(jnp.bfloat16)
        return jnp.dot(kmat, profile.reshape(-1), preferred_element_type=jnp.float32)

    indices = jnp.arange(SCANS, dtype=jnp.int32)
    return lax.map(one_scan, (indices, jacobian, lat_weight, centre, west, east, lat_offset, lev_offset))
```

```python
import functools

import jax
import jax.numpy as jnp
from jax import lax
from jax.experimental import pallas as pl
from jax.experimental.pallas import tpu as pltpu
from jax.sharding import PartitionSpec as P

BLAT = 8
BLEV = 32
AXES = ("lon", "lat")


def select_kernel(count, band_ref, meta_ref, own_ref, pair_ref, mine_ref, other_ref):
    width, rows, _ = own_ref.shape
    half = mine_ref.shape[0]
    meta = jnp.transpose(meta_ref[...])[:count]
    band = band_ref[0]
    lat_first = meta[:, BLAT : BLAT + 1].astype(jnp.int32)
    lev_first = meta[:, BLAT + 1 : BLAT + 2].astype(jnp.int32)
    lane = lax.broadcasted_iota(jnp.int32, (count, 128), 1)

    def weights(first):
        offset = lane + first - lat_first
        total = jnp.zeros((count, 128), jnp.float32)
        for j in range(BLAT):
            total = jnp.where(offset == j, meta[:, j : j + 1], total)
        return total

    full = jnp.concatenate(
        [weights(band * rows), weights((band + 1 - 2 * lax.rem(band, 2)) * rows)], axis=1
    )
    high = full.astype(jnp.bfloat16)
    low = (full - high.astype(jnp.float32)).astype(jnp.bfloat16)
    left = jnp.concatenate([high, low], axis=0)
    index = lev_first + lax.rem(lane, BLEV)
    spot = lane // BLEV
    for q in range(width // 4):
        tile = None
        for h in range(2):
            c = 4 * q + 2 * h
            right = jnp.concatenate(
                [
                    jnp.concatenate([own_ref[c], pair_ref[c]], axis=0),
                    jnp.concatenate([own_ref[c + 1], pair_ref[c + 1]], axis=0),
                ],
                axis=1,
            )
            both = jnp.dot(left, right, preferred_element_type=jnp.float32)
            both = both[:count] + both[count:]
            for i in range(2):
                box = jnp.take_along_axis(both[:, 128 * i : 128 * i + 128], index, axis=1)
                tile = box if tile is None else jnp.where(spot == 2 * h + i, box, tile)
        tile_at = slice(128 * q, 128 * q + 128)
        for g in range(half // 16):
            mine_ref[16 * g : 16 * g + 16, tile_at] = tile[32 * g : 32 * g + 16]
            other_ref[16 * g : 16 * g + 16, tile_at] = tile[32 * g + 16 : 32 * g + 32]


def select(band, meta, own, pair, count):
    meta = jnp.pad(meta, ((0, 16 - meta.shape[0]), (0, 128 - meta.shape[1])))
    width = own.shape[0]
    out = jax.ShapeDtypeStruct((count // 2, width * BLEV), jnp.float32)
    vmem = pl.BlockSpec(memory_space=pltpu.VMEM)
    return pl.pallas_call(
        functools.partial(select_kernel, count),
        out_shape=(out, out),
        in_specs=[pl.BlockSpec(memory_space=pltpu.SMEM), vmem, vmem, vmem],
        out_specs=(vmem, vmem),
        compiler_params=pltpu.CompilerParams(vmem_limit_bytes=12 * 1024 * 1024),
        cost_estimate=pl.CostEstimate(
            flops=2 * count * 256 * 128 * width * 2, bytes_accessed=2 * 1024 * 1024, transcendentals=0
        ),
        name="select",
    )(band, meta, own, pair)


def contract_kernel(parts, info_ref, jac_ref, *refs):
    pieces, out_ref, prof_ref = refs[:parts], refs[parts], refs[parts + 1]
    slots, tangents, lanes = out_ref.shape[0], out_ref.shape[1], 128
    odd = info_ref[3, 0]
    for piece, place in zip(pieces, (lax.mul(odd, 2), 1, lax.mul(1 - odd, 2))):
        start = pl.multiple_of(place * 1024, 1024)
        prof_ref[:, pl.ds(start, 1024)] = piece[...].astype(jnp.float32)
    column = lax.broadcasted_iota(jnp.int32, (1, lanes), 1) // BLEV
    place = lax.broadcasted_iota(jnp.int32, (tangents, lanes), 1)
    result = jnp.zeros((tangents, lanes), jnp.float32)
    for s in range(slots):
        first = 32 + info_ref[0, s] - info_ref[1, s]
        last = 32 + info_ref[0, s] + info_ref[2, s]

        def step(t, total):
            at = pl.multiple_of(t * lanes, lanes)
            row = prof_ref[s : s + 1, pl.ds(at, lanes)]
            r = column + 4 * t
            row = jnp.where((r >= first) & (r <= last), row, 0.0)
            return total + jac_ref[s, :, pl.ds(at, lanes)].astype(jnp.float32) * row

        total = lax.fori_loop(
            first // 4, last // 4 + 1, step, jnp.zeros((tangents, lanes), jnp.float32)
        )
        result = jnp.where(place == s, jnp.sum(total, axis=1, keepdims=True), result)
    out_ref[...] = jnp.transpose(result)[:slots]


def contract(info, jacobian, far, own, near):
    slots, tangents, depth = jacobian.shape
    vmem = pl.BlockSpec(memory_space=pltpu.VMEM)
    return pl.pallas_call(
        functools.partial(contract_kernel, 3),
        out_shape=jax.ShapeDtypeStruct((slots, tangents), jnp.float32),
        in_specs=[pl.BlockSpec(memory_space=pltpu.SMEM)] + [vmem] * 4,
        out_specs=vmem,
        scratch_shapes=[pltpu.VMEM((slots, depth), jnp.float32)],
        compiler_params=pltpu.CompilerParams(vmem_limit_bytes=20 * 1024 * 1024),
        cost_estimate=pl.CostEstimate(flops=2 * slots * tangents * depth, bytes_accessed=12582912, transcendentals=0),
        name="contract",
    )(info, jacobian, far, own, near)


def local(increment, jacobian, lat_weight, centre, west, east, lat_offset, lev_offset):
    n_lon, n_lat = lax.axis_size("lon"), lax.axis_size("lat")
    band = lax.axis_index("lat")
    odd = lax.rem(lax.axis_index("lon"), 2)

    def within(flip):
        return [(a * n_lat + b, a * n_lat + (b ^ flip)) for a in range(n_lon) for b in range(n_lat)]

    def swaps(start):
        pairs = [(a % n_lon, (a + 1) % n_lon) for a in range(start, n_lon, 2)]
        return pairs + [(b, a) for a, b in pairs]

    def across(value):
        return lax.ppermute(value, AXES, within(2))

    meta = jnp.concatenate(
        [
            lat_weight.T,
            lat_offset[None].astype(jnp.float32),
            lev_offset[None].astype(jnp.float32),
        ],
        axis=0,
    )
    meta = jnp.concatenate([meta, across(meta)], axis=1)
    pair = lax.ppermute(increment, AXES, within(1))
    meta_far = lax.ppermute(meta, "lon", swaps(1))
    meta_near = lax.ppermute(meta, "lon", swaps(0))
    bands = band[None].astype(jnp.int32)

    mine, other = select(bands, jnp.concatenate([meta, meta_near], axis=1), increment, pair, 64)
    near = (mine + across(other)).astype(jnp.bfloat16)
    own, near = near[:16], lax.ppermute(near[16:], "lon", swaps(0))
    mine, other = select(bands, meta_far, increment, pair, 32)
    far = lax.ppermute((mine + across(other)).astype(jnp.bfloat16), "lon", swaps(1))

    info = jnp.stack([centre, west, east, jnp.broadcast_to(odd, centre.shape).astype(jnp.int32)])
    return contract(info, jacobian, far, own, near)


def solution(mesh):
    return jax.shard_map(
        local,
        mesh=mesh,
        in_specs=(
            P("lon", "lat", None),
            P(("lon", "lat"), None, None),
            P(("lon", "lat"), None),
            P(("lon", "lat")),
            P(("lon", "lat")),
            P(("lon", "lat")),
            P(("lon", "lat")),
            P(("lon", "lat")),
        ),
        out_specs=P(("lon", "lat"), None),
        check_vma=False,
    )
```

```python
import jax
import jax.numpy as jnp
from jax import lax
from jax.experimental import pallas as pl
from jax.experimental.pallas import tpu as pltpu
from jax.sharding import PartitionSpec as P


BLAT = 8
BLEV = 32
LANES = 128
COLS = LANES // BLEV
AXES = ("lon", "lat")
VMEM = pl.BlockSpec(memory_space=pltpu.VMEM)
SMEM = pl.BlockSpec(memory_space=pltpu.SMEM)


def select_kernel(meta_ref, own_ref, pair_ref, *outs):
    width, rows = own_ref.shape[0], own_ref.shape[1]
    groups = len(outs) // 2
    count = 32 * groups
    meta = jnp.transpose(meta_ref[...])[:count]
    band = lax.axis_index("lat")
    lat_first, lev_first = [meta[:, BLAT + i : BLAT + i + 1].astype(jnp.int32) for i in range(2)]
    lane = lax.broadcasted_iota(jnp.int32, (count, LANES), 1)

    def weights(first):
        offset = lane + first - lat_first
        total = jnp.zeros((count, LANES), jnp.float32)
        for j in range(BLAT):
            total = jnp.where(offset == j, meta[:, j : j + 1], total)
        return total

    full = jnp.concatenate(
        [weights(band * rows), weights((band + 1 - 2 * lax.rem(band, 2)) * rows)], axis=1
    )
    high = full.astype(jnp.bfloat16)
    low = (full - high.astype(jnp.float32)).astype(jnp.bfloat16)
    left = jnp.concatenate([high, low], axis=0)
    index = lev_first + lax.rem(lane, BLEV)
    spot = lane // BLEV
    for q in range(width // COLS):
        tile = None
        for h in range(COLS // 2):
            c = COLS * q + 2 * h
            right = jnp.concatenate(
                [
                    jnp.concatenate([own_ref[c], pair_ref[c]], axis=0),
                    jnp.concatenate([own_ref[c + 1], pair_ref[c + 1]], axis=0),
                ],
                axis=1,
            )
            both = jnp.dot(left, right, preferred_element_type=jnp.float32)
            both = both[:count] + both[count:]
            for i in range(2):
                box = jnp.take_along_axis(both[:, LANES * i : LANES * (i + 1)], index, axis=1)
                tile = box if tile is None else jnp.where(spot == 2 * h + i, box, tile)
        at = slice(LANES * q, LANES * (q + 1))
        for g in range(groups):
            outs[2 * g][:, at] = tile[32 * g : 32 * g + 16]
            outs[2 * g + 1][:, at] = tile[32 * g + 16 : 32 * g + 32]


def select(meta, own, pair):
    count = meta.shape[1]
    width = own.shape[0]
    meta = jnp.pad(meta, ((0, 0), (0, LANES - count)))
    out = jax.ShapeDtypeStruct((16, width * BLEV), jnp.float32)
    outs = count // 16
    return pl.pallas_call(
        select_kernel,
        out_shape=(out,) * outs,
        in_specs=[VMEM] * 3,
        out_specs=(VMEM,) * outs,
        compiler_params=pltpu.CompilerParams(vmem_limit_bytes=12 * 1024 * 1024),
        cost_estimate=pl.CostEstimate(
            flops=5 * 10**9, bytes_accessed=2 * 1024 * 1024, transcendentals=0
        ),
    )(meta, own, pair)


def stage_kernel(own_ref, info_ref, own_out, info_out, low_out, high_out):
    own_out[...] = own_ref[...]
    info_out[...] = info_ref[...]
    slots = low_out.shape[0]
    bounds = jnp.transpose(info_ref[...])[:slots]
    low_out[...] = jnp.broadcast_to(bounds[:, :1], low_out.shape)
    high_out[...] = jnp.broadcast_to(bounds[:, 1:2], high_out.shape)


def stage(increment, info, slots):
    bound = jax.ShapeDtypeStruct((slots, LANES), info.dtype)
    return pl.pallas_call(
        stage_kernel,
        out_shape=(
            jax.ShapeDtypeStruct(increment.shape, increment.dtype),
            jax.ShapeDtypeStruct(info.shape, info.dtype),
            bound,
            bound,
        ),
        in_specs=[VMEM, VMEM],
        out_specs=(VMEM,) * 4,
        compiler_params=pltpu.CompilerParams(vmem_limit_bytes=8 * 1024 * 1024),
        cost_estimate=pl.CostEstimate(flops=10**7, bytes_accessed=2**21, transcendentals=0),
        name="stage",
    )(increment, info)


def masked(piece, third, low_ref, high_ref):
    slots, depth = piece.shape
    column = lax.broadcasted_iota(jnp.int32, (slots, LANES), 1) // BLEV
    tiles = []
    for q in range(depth // LANES):
        r = column + COLS * q + third * (depth // BLEV)
        keep = (r >= low_ref[...]) & (r <= high_ref[...])
        part = piece[:, LANES * q : LANES * (q + 1)].astype(jnp.float32)
        tiles.append(jnp.where(keep, part, 0.0))
    return jnp.concatenate(tiles, axis=1)


def tile_product(jac_ref, prof_ref, s, t, base):
    row = prof_ref[s : s + 1, pl.ds(pl.multiple_of((t - base) * LANES, LANES), LANES)]
    tile = jac_ref[s, :, pl.ds(pl.multiple_of(t * LANES, LANES), LANES)]
    return tile.astype(jnp.float32) * row


def near_contract_kernel(info_ref, low_ref, high_ref, jac_ref, own_ref, near_ref, acc_ref, prof_ref):
    slots, depth = own_ref.shape
    odd = lax.rem(lax.axis_index("lon"), 2)
    start = pl.multiple_of((1 - odd) * depth, depth)
    prof_ref[:, pl.ds(pl.multiple_of(odd * depth, depth), depth)] = masked(
        own_ref[...], 1, low_ref, high_ref
    )
    prof_ref[:, pl.ds(start, depth)] = masked(near_ref[...], 2 - 2 * odd, low_ref, high_ref)
    zero = jnp.zeros(acc_ref.shape[1:], jnp.float32)
    base = 8 * (1 - odd)
    unroll, shift = 4, 4
    for s in range(slots):
        first = lax.max(info_ref[0, s], COLS * base)
        last = lax.min(info_ref[1, s], COLS * (base + 16) - 1)

        def step(g, total):
            for i in range(unroll):
                total = total + tile_product(jac_ref, prof_ref, s, unroll * g + i, base)
            return total

        acc_ref[s] = lax.fori_loop(
            lax.shift_right_arithmetic(first, shift), lax.shift_right_arithmetic(last, shift) + 1, step, zero
        )


def near_contract(info, low, high, jacobian, own, near):
    slots, depth = own.shape
    tangents = jacobian.shape[1]
    return pl.pallas_call(
        near_contract_kernel,
        out_shape=jax.ShapeDtypeStruct((slots, tangents, LANES), jnp.float32),
        in_specs=[SMEM] + [VMEM] * 5,
        out_specs=VMEM,
        scratch_shapes=[pltpu.VMEM((slots, 2 * depth), jnp.float32)],
        compiler_params=pltpu.CompilerParams(vmem_limit_bytes=20 * 1024 * 1024),
        cost_estimate=pl.CostEstimate(
            flops=4 * slots * tangents * depth, bytes_accessed=4 * slots * tangents * depth, transcendentals=0
        ),
        name="near_contract",
    )(info, low, high, jacobian, own, near)


def far_contract_kernel(low_ref, high_ref, jac_ref, far_ref, acc_ref, out_ref, prof_ref):
    slots, tangents = out_ref.shape
    odd = lax.rem(lax.axis_index("lon"), 2)
    base = 16 * odd
    prof_ref[...] = masked(far_ref[...], 2 * odd, low_ref, high_ref)
    place = lax.broadcasted_iota(jnp.int32, (tangents, LANES), 1)
    result = jnp.zeros((tangents, LANES), jnp.float32)
    for s in range(slots):
        total = acc_ref[s]
        for u in range(8):
            total = total + tile_product(jac_ref, prof_ref, s, base + u, base)
        result = jnp.where(place == s, jnp.sum(total, axis=1, keepdims=True), result)
    out_ref[...] = jnp.transpose(result)[:slots]


def far_contract(low, high, jacobian, far, acc):
    slots, depth = far.shape
    tangents = jacobian.shape[1]
    return pl.pallas_call(
        far_contract_kernel,
        out_shape=jax.ShapeDtypeStruct((slots, tangents), jnp.float32),
        in_specs=[VMEM] * 5,
        out_specs=VMEM,
        scratch_shapes=[pltpu.VMEM((slots, depth), jnp.float32)],
        compiler_params=pltpu.CompilerParams(vmem_limit_bytes=24 * 1024 * 1024),
        cost_estimate=pl.CostEstimate(
            flops=2 * slots * tangents * depth, bytes_accessed=2 * slots * tangents * depth, transcendentals=0
        ),
        name="far_contract",
    )(low, high, jacobian, far, acc)


def local(increment, jacobian, lat_weight, centre, west, east, lat_offset, lev_offset):
    n_lon, n_lat = lax.axis_size("lon"), lax.axis_size("lat")
    slots = centre.shape[0]

    def within(flip):
        return [(a * n_lat + b, a * n_lat + (b ^ flip)) for a in range(n_lon) for b in range(n_lat)]

    def swaps(start):
        pairs = [(a % n_lon, (a + 1) % n_lon) for a in range(start, n_lon, 2)]
        return pairs + [(b, a) for a, b in pairs]

    def across(value):
        return lax.ppermute(value, AXES, within(2))

    meta = jnp.concatenate(
        [lat_weight.T, lat_offset[None].astype(jnp.float32), lev_offset[None].astype(jnp.float32)], axis=0
    )
    meta = lax.optimization_barrier(jnp.pad(meta, ((0, BLAT - 2), (0, 0))))
    meta_y = across(meta)
    pair = lax.ppermute(increment, AXES, within(1))
    info = jnp.pad(jnp.stack([32 + centre - west, 32 + centre + east]), ((0, 6), (0, LANES - slots)))
    inc, info, low, high = stage(increment, info, slots)
    meta = lax.optimization_barrier(jnp.concatenate([meta, meta_y], axis=1))
    meta_far = lax.ppermute(meta, "lon", swaps(1))
    meta_near = lax.ppermute(meta, "lon", swaps(0))

    own, own_other, near, near_other = select(jnp.concatenate([meta, meta_near], axis=1), inc, pair)
    near_other = across(near_other)
    near = (near + near_other).astype(jnp.bfloat16)
    near = lax.ppermute(near, "lon", swaps(0))
    far, far_other = select(meta_far, inc, pair)
    far_other = across(far_other)
    own_other = across(own_other)
    own = (own + own_other).astype(jnp.bfloat16)
    far = (far + far_other).astype(jnp.bfloat16)
    far = lax.ppermute(far, "lon", swaps(1))
    acc = near_contract(info, low, high, jacobian, own, near)
    return far_contract(low, high, jacobian, far, acc)


def solution(mesh):
    return jax.shard_map(
        local,
        mesh=mesh,
        in_specs=(
            P("lon", "lat", None),
            P(("lon", "lat"), None, None),
            P(("lon", "lat"), None),
            P(("lon", "lat")),
            P(("lon", "lat")),
            P(("lon", "lat")),
            P(("lon", "lat")),
            P(("lon", "lat")),
        ),
        out_specs=P(("lon", "lat"), None),
        check_vma=False,
    )
```

```python
import functools

import jax
import jax.numpy as jnp
from jax import lax
from jax.experimental import pallas as pl
from jax.experimental.pallas import tpu as pltpu
from jax.sharding import PartitionSpec as P


BLAT = 8
BLEV = 32
LANES = 128
COLS = LANES // BLEV
AXES = ("lon", "lat")
VMEM = pl.BlockSpec(memory_space=pltpu.VMEM)


def select_kernel(keep, meta_ref, own_ref, pair_ref, *outs):
    if keep:
        outs[-1][...] = own_ref[...]
        outs = outs[:-1]
    width, rows = own_ref.shape[0], own_ref.shape[1]
    groups = len(outs) // 2
    count = 32 * groups
    meta = jnp.transpose(meta_ref[...])[:count]
    band = lax.axis_index("lat")
    lat_first, lev_first = [meta[:, BLAT + i : BLAT + i + 1].astype(jnp.int32) for i in range(2)]
    lane = lax.broadcasted_iota(jnp.int32, (count, LANES), 1)

    def weights(first):
        offset = lane + first - lat_first
        total = jnp.zeros((count, LANES), jnp.float32)
        for j in range(BLAT):
            total = jnp.where(offset == j, meta[:, j : j + 1], total)
        return total

    full = jnp.concatenate(
        [weights(band * rows), weights((band + 1 - 2 * lax.rem(band, 2)) * rows)], axis=1
    )
    high = full.astype(jnp.bfloat16)
    low = (full - high.astype(jnp.float32)).astype(jnp.bfloat16)
    left = jnp.concatenate([high, low], axis=0)
    index = lev_first + lax.rem(lane, BLEV)
    spot = lane // BLEV
    for q in range(width // COLS):
        tile = None
        for h in range(COLS // 2):
            c = COLS * q + 2 * h
            right = jnp.concatenate(
                [
                    jnp.concatenate([own_ref[c], pair_ref[c]], axis=0),
                    jnp.concatenate([own_ref[c + 1], pair_ref[c + 1]], axis=0),
                ],
                axis=1,
            )
            both = jnp.dot(left, right, preferred_element_type=jnp.float32)
            both = both[:count] + both[count:]
            for i in range(2):
                box = jnp.take_along_axis(both[:, LANES * i : LANES * (i + 1)], index, axis=1)
                tile = box if tile is None else jnp.where(spot == 2 * h + i, box, tile)
        at = slice(LANES * q, LANES * (q + 1))
        for g in range(groups):
            outs[2 * g][:, at] = tile[32 * g : 32 * g + 16]
            outs[2 * g + 1][:, at] = tile[32 * g + 16 : 32 * g + 32]


def select(meta, own, pair, keep):
    count = meta.shape[1]
    width = own.shape[0]
    meta = jnp.pad(meta, ((0, 0), (0, LANES - count)))
    out = jax.ShapeDtypeStruct((16, width * BLEV), jnp.float32)
    outs = (out,) * (count // 16)
    if keep:
        outs += (jax.ShapeDtypeStruct(own.shape, own.dtype),)
    return pl.pallas_call(
        functools.partial(select_kernel, keep),
        out_shape=outs,
        in_specs=[VMEM] * 3,
        out_specs=(VMEM,) * len(outs),
        compiler_params=pltpu.CompilerParams(vmem_limit_bytes=12 * 1024 * 1024),
        cost_estimate=pl.CostEstimate(
            flops=5 * 10**9, bytes_accessed=2 * 1024 * 1024, transcendentals=0
        ),
    )(meta, own, pair)


def limits_kernel(info_ref, low_out, high_out):
    slots = low_out.shape[0]
    bounds = jnp.transpose(info_ref[...])[:slots]
    low_out[...] = jnp.broadcast_to(bounds[:, :1], low_out.shape)
    high_out[...] = jnp.broadcast_to(bounds[:, 1:2], high_out.shape)


def limits(info, slots):
    bound = jax.ShapeDtypeStruct((slots, LANES), info.dtype)
    return pl.pallas_call(
        limits_kernel,
        out_shape=(bound, bound),
        in_specs=[VMEM],
        out_specs=(VMEM, VMEM),
        compiler_params=pltpu.CompilerParams(vmem_limit_bytes=4 * 1024 * 1024),
        name="limits",
    )(info)


def mark_kernel(meta_ref, out_ref):
    out_ref[...] = meta_ref[...]


def mark(meta):
    return pl.pallas_call(
        mark_kernel,
        out_shape=jax.ShapeDtypeStruct(meta.shape, meta.dtype),
        in_specs=[VMEM],
        out_specs=VMEM,
        compiler_params=pltpu.CompilerParams(vmem_limit_bytes=4 * 1024 * 1024),
        cost_estimate=pl.CostEstimate(flops=5 * 10**9, bytes_accessed=2**14, transcendentals=0),
        name="mark",
    )(meta)


def masked(piece, third, low_ref, high_ref):
    slots, depth = piece.shape
    column = lax.broadcasted_iota(jnp.int32, (slots, LANES), 1) // BLEV
    tiles = []
    for q in range(depth // LANES):
        r = column + COLS * q + third * (depth // BLEV)
        keep = (r >= low_ref[...]) & (r <= high_ref[...])
        part = piece[:, LANES * q : LANES * (q + 1)].astype(jnp.float32)
        tiles.append(jnp.where(keep, part, 0.0).astype(jnp.bfloat16))
    return jnp.concatenate(tiles, axis=1)


def scan_rows(jac_ref, profile, third, start):
    slots, depth = profile.shape
    row = lax.broadcasted_iota(jnp.int32, start.shape, 0)
    at = pl.ds(pl.multiple_of(third * depth, depth), depth)
    rows = start
    for s in range(slots):
        product = lax.dot_general(
            profile, jac_ref[s, :, at], (((1,), (1,)), ((), ())), preferred_element_type=jnp.float32
        )
        rows = jnp.where(row == s, rows + product, rows)
    return rows


def near_contract_kernel(low_ref, high_ref, jac_ref, own_ref, near_ref, part_ref):
    odd = lax.rem(lax.axis_index("lon"), 2)
    rows = jnp.zeros(part_ref.shape, jnp.float32)
    for piece, third in ((own_ref, 1), (near_ref, 2 - 2 * odd)):
        profile = masked(piece[...], third, low_ref, high_ref)
        rows = scan_rows(jac_ref, profile, third, rows)
    part_ref[...] = rows


def far_contract_kernel(low_ref, high_ref, jac_ref, far_ref, part_ref, out_ref):
    third = 2 * lax.rem(lax.axis_index("lon"), 2)
    profile = masked(far_ref[...], third, low_ref, high_ref)
    out_ref[...] = scan_rows(jac_ref, profile, third, part_ref[...])


def contract(kernel, jacobian, *operands):
    slots, tangents, depth = jacobian.shape
    return pl.pallas_call(
        kernel,
        out_shape=jax.ShapeDtypeStruct((slots, tangents), jnp.float32),
        in_specs=[VMEM] * (1 + len(operands)),
        out_specs=VMEM,
        compiler_params=pltpu.CompilerParams(vmem_limit_bytes=20 * 1024 * 1024),
        cost_estimate=pl.CostEstimate(
            flops=4 * slots * tangents * depth, bytes_accessed=4 * slots * tangents * depth, transcendentals=0
        ),
    )(*operands[:2], jacobian, *operands[2:])


def local(increment, jacobian, lat_weight, centre, west, east, lat_offset, lev_offset):
    n_lon, n_lat = lax.axis_size("lon"), lax.axis_size("lat")
    slots = centre.shape[0]

    def within(flip):
        return [(a * n_lat + b, a * n_lat + (b ^ flip)) for a in range(n_lon) for b in range(n_lat)]

    def swaps(start):
        pairs = [(a % n_lon, (a + 1) % n_lon) for a in range(start, n_lon, 2)]
        return pairs + [(b, a) for a, b in pairs]

    def crossed(start, flip):
        return [(a * n_lat + b, c * n_lat + (b ^ flip)) for a, c in swaps(start) for b in range(n_lat)]

    def across(value):
        return lax.ppermute(value, AXES, within(2))

    meta = jnp.concatenate(
        [lat_weight.T, lat_offset[None].astype(jnp.float32), lev_offset[None].astype(jnp.float32)], axis=0
    )
    meta = mark(jnp.pad(meta, ((0, BLAT - 2), (0, 0))))
    meta_y = across(meta)
    near_a = lax.ppermute(meta, AXES, crossed(0, 0))
    near_b = lax.ppermute(meta, AXES, crossed(0, 2))
    pair = lax.ppermute(increment, AXES, within(1))
    meta = lax.optimization_barrier(jnp.concatenate([meta, meta_y], axis=1))
    meta_far = lax.ppermute(meta, "lon", swaps(1))

    own, own_other, near, near_other, inc = select(
        jnp.concatenate([meta, near_a, near_b], axis=1), increment, pair, True
    )
    near_other = across(near_other)
    near = (near + near_other).astype(jnp.bfloat16)
    near = lax.ppermute(near, "lon", swaps(0))
    far, far_other = select(meta_far, inc, pair, False)
    far_other = across(far_other)
    info = jnp.pad(jnp.stack([32 + centre - west, 32 + centre + east]), ((0, 6), (0, LANES - slots)))
    low, high = limits(info, slots)
    own_other = across(own_other)
    own = (own + own_other).astype(jnp.bfloat16)
    far = (far + far_other).astype(jnp.bfloat16)
    far = lax.ppermute(far, "lon", swaps(1))
    part = contract(near_contract_kernel, jacobian, low, high, own, near)
    return contract(far_contract_kernel, jacobian, low, high, far, part)


def solution(mesh):
    return jax.shard_map(
        local,
        mesh=mesh,
        in_specs=(
            P("lon", "lat", None),
            P(("lon", "lat"), None, None),
            P(("lon", "lat"), None),
            P(("lon", "lat")),
            P(("lon", "lat")),
            P(("lon", "lat")),
            P(("lon", "lat")),
            P(("lon", "lat")),
        ),
        out_specs=P(("lon", "lat"), None),
        check_vma=False,
    )
```
